32 devices in a mesh: dev: 8 (over z, x), rep: 4 (over y, core).
Axes of the slice: x: 2, y: 2, z: 4, core: 2. Of those that a mesh axis runs over, the one named last changes fastest.
Arguments:
- h_zero: bfloat16 [32768, 256], P(('dev', 'rep')), may hold values from 0 to 2
- h_prev: bfloat16 [32768, 256], P(('dev', 'rep')), may hold values from 0 to 2
- hist_a: bfloat16 [32768, 256], P('dev'), may hold values from 0 to 2
- hist_b: bfloat16 [32768, 256], P('dev'), may hold values from 0 to 2
- tile_vals: bfloat16 [256, 12, 128, 128], P(('dev', 'rep'))
- tile_cols: int32 [256, 12], P(('dev', 'rep')), may hold values from 0 to 47, as said below
- pull_rows: int32 [32, 8, 128], P(('dev', 'rep')), may hold values from 0 to 4095
- pull_counts: int32 [32, 8], P(('dev', 'rep')), may hold values from 96 to 128, as said below
- weight_two: bfloat16 [256, 256], replicated, may hold values from -0.375 to 0.375
- weight_three: bfloat16 [256, 256], replicated, may hold values from -0.375 to 0.375
- grad_out: bfloat16 [32768, 256], P(('dev', 'rep')), may hold values from -0.125 to 0.125
Outputs:
- layer_three: bfloat16 [32768, 256], P(('dev', 'rep'))
- new_history: bfloat16 [32768, 256], P('dev')
- weight_grad: float32 [256, 256], replicated
The draws below stay inside these ranges and needn't reach their ends.
Inputs may be any that keep to these rules, and one draw needn't show every extreme that they name: `tile_cols`: entry 0 of a row block names one of its device's own 8 blocks; entries 1 to 3 name blocks of the owner's history shard; the other 8 name pulled blocks of consecutive owners modulo 8, and every owner's block is named by some row block of each device. `pull_rows`: entries at slots at or past the block's count are read by no output. `pull_counts`: every device pulls a full block of 128 rows from some owner and a block of exactly 96 rows from another.
All inputs are finite; a program needn't handle non-finite values.
Results may differ from the reference program's by a relative error of at most 0.0034.
Values may be sent and summed in bfloat16 or wider, within the bound.
A program may use at most 128 MiB of HBM per device.

```python
import math
import jax
import jax.numpy as jnp
from jax import lax

WIDTH = 256
BATCH = 1024
TILE = 128
HOME_TILES = 3
REMOTE_TILES = 8
TPR = 12
ROWBLK = 8
WORKERS = 32
SHARD = 4096
NODES = 32768
N_DEV = 8
N_REP = 4


def draw_tile_vals(key, part):
    full_shape = (WORKERS * ROWBLK, TPR, TILE, TILE)
    key_mask, key_value = jax.random.split(key, 2)
    edge_mask = jax.random.bernoulli(key_mask, 0.125, full_shape).astype(jnp.float32)
    edge_weight = jax.random.uniform(key_value, full_shape, jnp.float32, 0.5, 1.5)
    return (edge_mask * edge_weight * (8.0 / (TPR * TILE))).astype(jnp.bfloat16)


def draw_tile_cols(key, part):
    key_local, key_home, key_shift = jax.random.split(key, 3)
    row_count = WORKERS * ROWBLK
    local_cols = jax.random.randint(key_local, (row_count, 1), 0, ROWBLK, jnp.int32)
    home_cols = jax.random.randint(key_home, (row_count, HOME_TILES), ROWBLK, ROWBLK + N_REP * ROWBLK, jnp.int32)
    shifts = jax.random.randint(key_shift, (WORKERS, 1), 0, N_DEV, jnp.int32)
    shift_rows = jnp.repeat(shifts, ROWBLK, axis=0)
    block_pos = (jnp.arange(row_count, dtype=jnp.int32) % ROWBLK)[:, None]
    slot_pos = jnp.arange(REMOTE_TILES, dtype=jnp.int32)[None, :]
    peer_ids = (block_pos * REMOTE_TILES + slot_pos + shift_rows) % N_DEV
    remote_cols = ROWBLK + N_REP * ROWBLK + peer_ids
    return jnp.concatenate([local_cols, home_cols, remote_cols], axis=1).astype(jnp.int32)


def draw_pull_counts(key, part):
    key_one, key_two, key_full = jax.random.split(key, 3)
    full_shape = (WORKERS, N_DEV)
    first = jax.random.randint(key_one, full_shape, 1, TILE + 1, jnp.int32)
    second = jax.random.randint(key_two, full_shape, 1, TILE + 1, jnp.int32)
    counts = TILE - first * second // (4 * TILE)
    offset = jax.random.randint(key_full, (), 0, N_DEV, jnp.int32)
    full_peer = (jnp.arange(WORKERS, dtype=jnp.int32) * 5 + offset) % N_DEV
    low_peer = (full_peer + 1) % N_DEV
    peer_ids = jnp.arange(N_DEV, dtype=jnp.int32)[None, :]
    counts = jnp.where(peer_ids == low_peer[:, None], TILE - TILE // 4, counts)
    counts = jnp.where(peer_ids == full_peer[:, None], TILE, counts)
    return counts.astype(jnp.int32)


def set_ends(drawn, stream_key, low, top_value):
    spot = [jax.random.randint(jax.random.fold_in(stream_key, axis), (), 0, length) for axis, length in enumerate(drawn.shape)]
    longest = drawn.shape.index(max(drawn.shape))
    next_to = spot[:longest] + [(spot[longest] + 1) % drawn.shape[longest]] + spot[longest + 1:]
    return drawn.at[tuple(spot)].set(low).at[tuple(next_to)].set(top_value)


def levels(rng, dims, cuts, low, top_value):
    gain = 1.0
    for axis_at, parts in cuts:
        draws = jax.random.uniform(jax.random.fold_in(jax.random.fold_in(rng, 6), axis_at), (parts,), jnp.float32, low / len(cuts), top_value / len(cuts))
        gain = gain * jnp.repeat(jnp.exp(draws), dims[axis_at] // parts).reshape((-1,) + (1,) * (len(dims) - 1 - axis_at))
    return gain


def gaussian(key, extent, spread, most, pieces=(), kind=jnp.bfloat16):
    level = levels(key, extent, pieces, -0.22, 0.18) if pieces else 1.0
    entries = jax.random.normal(key, extent, jnp.float32) * spread * level
    return jnp.minimum(jnp.maximum(entries, -most), most).astype(kind)


def setup_inputs(seed: int = 0) -> dict:
    key_list = jax.random.split(jax.random.key(seed), 12)
    return {
        "h_zero": jnp.clip(2.0 * jax.random.uniform(key_list[0], (NODES, WIDTH), jnp.float32) ** levels(key_list[0], (NODES, WIDTH), ((0, 32),), -0.2, 0.2), 0.0, 2.0).astype(jnp.bfloat16),
        "h_prev": jnp.clip(2.0 * jax.random.uniform(key_list[1], (NODES, WIDTH), jnp.float32) ** levels(key_list[1], (NODES, WIDTH), ((0, 32),), -0.2, 0.2), 0.0, 2.0).astype(jnp.bfloat16),
        "hist_a": jnp.clip(2.0 * jax.random.uniform(key_list[2], (NODES, WIDTH), jnp.float32) ** levels(key_list[2], (NODES, WIDTH), ((0, 8),), -0.2, 0.2), 0.0, 2.0).astype(jnp.bfloat16),
        "hist_b": jnp.clip(2.0 * jax.random.uniform(key_list[3], (NODES, WIDTH), jnp.float32) ** levels(key_list[3], (NODES, WIDTH), ((0, 8),), -0.2, 0.2), 0.0, 2.0).astype(jnp.bfloat16),
        "tile_vals": draw_tile_vals(jax.random.fold_in(key_list[11], 71), 0),
        "tile_cols": draw_tile_cols(jax.random.fold_in(key_list[11], 71), 0),
        "pull_rows": set_ends(jax.random.randint(key_list[6], (WORKERS, N_DEV, TILE), 0, SHARD), jax.random.fold_in(key_list[6], 1), 0, SHARD - 1).astype(jnp.int32),
        "pull_counts": draw_pull_counts(jax.random.fold_in(key_list[11], 71), 0),
        "weight_two": gaussian(key_list[8], (WIDTH, WIDTH), WIDTH ** -0.5, 0.375),
        "weight_three": gaussian(key_list[9], (WIDTH, WIDTH), WIDTH ** -0.5, 0.375),
        "grad_out": gaussian(key_list[10], (NODES, WIDTH), (4.0 / NODES ** 0.5), 0.125, ((0, 32),)),
    }


restart = 0.1
strength = 0.5


def propagate(current, history, pulled, values, columns, start_rows, weight, layer_number):
    feature_width = current.shape[1]
    source = jnp.concatenate([current, history, pulled.reshape(-1, feature_width)], axis=0)
    blocks = source.reshape(-1, TILE, feature_width)
    picked = jnp.take(blocks, columns.reshape(-1), axis=0).reshape(columns.shape + (TILE, feature_width))
    summed = jnp.einsum("btij,btjf->bif", values.astype(jnp.float32), picked.astype(jnp.float32))
    summed = summed.reshape(current.shape[0], feature_width)
    mixed_rows = (1.0 - restart) * summed + restart * start_rows.astype(jnp.float32)
    mixed_low = mixed_rows.astype(jnp.bfloat16)
    factor = math.log(strength / layer_number + 1.0)
    product = jnp.dot(mixed_low, weight, preferred_element_type=jnp.float32)
    inner_sum = (1.0 - factor) * mixed_rows + factor * product
    return jnp.maximum(inner_sum, 0.0).astype(jnp.bfloat16), mixed_low


def reference(h_zero, h_prev, hist_a, hist_b, tile_vals, tile_cols, pull_rows, pull_counts, weight_two, weight_three, grad_out):
    shard_a = hist_a.reshape(N_DEV, SHARD, WIDTH)
    shard_b = hist_b.reshape(N_DEV, SHARD, WIDTH)
    owners = jnp.arange(N_DEV, dtype=jnp.int32)[:, None]
    slot_ids = jnp.arange(TILE, dtype=jnp.int32)[None, :]

    def device(items):
        worker, start_rows, current, values, columns, wanted, counts, upstream = items
        home_shard = (worker // N_REP).astype(jnp.int32)
        live_mask = (slot_ids < counts[:, None])[:, :, None]
        pulled_a = jnp.where(live_mask, shard_a[owners, wanted], jnp.zeros((), shard_a.dtype))
        pulled_b = jnp.where(live_mask, shard_b[owners, wanted], jnp.zeros((), shard_b.dtype))
        own_a = lax.dynamic_index_in_dim(shard_a, home_shard, 0, keepdims=False)
        own_b = lax.dynamic_index_in_dim(shard_b, home_shard, 0, keepdims=False)
        second, unused_mix = propagate(current, own_a, pulled_a, values, columns, start_rows, weight_two, 2)
        layer_out, mixed_low = propagate(second, own_b, pulled_b, values, columns, start_rows, weight_three, 3)
        factor = math.log(strength / 3 + 1.0)
        grad_term = factor * jnp.dot(mixed_low.T, upstream, preferred_element_type=jnp.float32)
        return layer_out, second, grad_term

    items = (
        jnp.arange(WORKERS, dtype=jnp.int32),
        h_zero.reshape(WORKERS, BATCH, WIDTH),
        h_prev.reshape(WORKERS, BATCH, WIDTH),
        tile_vals.reshape(WORKERS, ROWBLK, TPR, TILE, TILE),
        tile_cols.reshape(WORKERS, ROWBLK, TPR),
        pull_rows,
        pull_counts,
        grad_out.reshape(WORKERS, BATCH, WIDTH),
    )
    layer_out, second, grad_terms = lax.map(device, items)
    return layer_out.reshape(NODES, WIDTH), second.reshape(NODES, WIDTH), jnp.sum(grad_terms, axis=0)
```

```python
import functools
import math

import jax
import jax.numpy as jnp
from jax import lax
from jax.experimental import pallas as pl
from jax.experimental.pallas import tpu as pltpu
from jax.sharding import PartitionSpec as P

restart = 0.1
strength = 0.5
MESH = pl.DeviceIdType.MESH


def kernel(
    D, R,
    cols, counts, rows_in,
    h_zero, h_prev, hist_a, hist_b, tile_vals, w_two, w_three, grad_out,
    layer_out, hist_out, grad_res,
    zero_v, cur_v, hist_av, hist_bv, vals_v, w2_v, w3_v, up_v,
    ask, asked, col, send_a, send_b, pull_a, pull_b, acc, acc_a, acc_b,
    fresh, low_v, out_v, g_send, g_recv, g_part, g_all,
    local_sem, idx_s, idx_r, a_s, a_r, b_s, b_r, f_s, f_r, out_sem, g_s, g_r, p_s, p_r,
):
    N = D * R
    d = lax.axis_index("dev")
    r = lax.axis_index("rep")
    me = d * R + r
    slots = rows_in.shape[2]
    feat = hist_av.shape[2]
    blocks = vals_v.shape[0]
    tiles = vals_v.shape[1]
    home = 4
    home_blocks = hist_av.shape[0]

    loads = [
        (hist_a, hist_av), (tile_vals, vals_v), (h_prev, cur_v), (hist_b, hist_bv),
        (h_zero, zero_v), (w_two, w2_v), (w_three, w3_v), (grad_out, up_v),
    ]
    copies = [pltpu.make_async_copy(s, t, local_sem.at[i]) for i, (s, t) in enumerate(loads)]
    for c in copies:
        c.start()

    barrier = pltpu.get_barrier_semaphore()

    def greet(k, _):
        t = lax.rem(me + 1 + k, N)
        pl.semaphore_signal(
            barrier, inc=1, device_id=(lax.div(t, R), lax.rem(t, R)), device_id_type=MESH
        )
        return 0

    lax.fori_loop(0, N - 1, greet, 0)

    lane = lax.broadcasted_iota(jnp.int32, (1, slots), 1)

    def mask_rows(p, _):
        ask[p] = jnp.where(lane < counts[0, p], rows_in[0, pl.ds(p, 1), :], -1)
        return 0

    lax.fori_loop(0, D, mask_rows, 0)
    pl.semaphore_wait(barrier, N - 1)

    def send_rows(j, _):
        p = lax.rem(d + 1 + j, D)
        pltpu.make_async_remote_copy(
            src_ref=ask.at[p], dst_ref=asked.at[d], send_sem=idx_s, recv_sem=idx_r,
            device_id=(p, r), device_id_type=MESH,
        ).start()
        return 0

    lax.fori_loop(0, D - 1, send_rows, 0)
    asked[d] = ask[d]

    def whole(ref, n, s, q):
        part = ref.at[pl.ds(0, n)]
        return pltpu.make_async_remote_copy(
            src_ref=part, dst_ref=part, send_sem=s, recv_sem=q,
            device_id=(lax.rem(d + 1, D), r), device_id_type=MESH,
        )

    whole(asked, D - 1, idx_s, idx_r).wait_recv()

    def column(j, _):
        q = lax.rem(d + D - 1 - j + D, D)
        col[j] = jnp.broadcast_to(asked[q], (slots, slots)).T
        return 0

    lax.fori_loop(0, D, column, 0)

    group = 4 if D % 4 == 0 else 1
    chunk_blocks = 8
    depth = chunk_blocks * slots
    lanes = lax.broadcasted_iota(jnp.int32, (group * slots, depth), 1)

    def gather(table, send_buf, pull_buf, s, q_sem):
        def one_group(g, _):
            keys = col[pl.ds(g * group, group)].reshape(group * slots, slots)
            wide = jnp.concatenate([keys] * chunk_blocks, axis=1)

            def one_chunk(k, _):
                hot = jnp.where(wide - k * depth == lanes, 1.0, 0.0).astype(jnp.bfloat16)
                part = table[pl.ds(k * chunk_blocks, chunk_blocks)].reshape(depth, feat)
                found = jnp.dot(hot, part, preferred_element_type=jnp.float32)

                @pl.when(k == 0)
                def _():
                    acc[...] = found

                @pl.when(k > 0)
                def _():
                    acc[...] += found

                return 0

            lax.fori_loop(0, home_blocks // chunk_blocks, one_chunk, 0)
            send_buf[pl.ds(g * group, group)] = (
                acc[...].astype(jnp.bfloat16).reshape(group, slots, feat)
            )

            def send_one(i, _):
                j = g * group + i

                @pl.when(j < D - 1)
                def _():
                    q = lax.rem(d + D - 1 - j + D, D)
                    pltpu.make_async_remote_copy(
                        src_ref=send_buf.at[j], dst_ref=pull_buf.at[d], send_sem=s, recv_sem=q_sem,
                        device_id=(q, r), device_id_type=MESH,
                    ).start()

                return 0

            lax.fori_loop(0, group, send_one, 0)
            return 0

        lax.fori_loop(0, D // group, one_group, 0)
        pull_buf[d] = send_buf[D - 1]

    copies[0].wait()
    gather(hist_av, send_a, pull_a, a_s, a_r)
    copies[3].wait()
    gather(hist_bv, send_b, pull_b, b_s, b_r)
    for i in (1, 2, 4, 5, 6, 7):
        copies[i].wait()

    def product(i, picks):
        left = jnp.concatenate([vals_v[i, t] for t, _ in picks], axis=1)
        right = jnp.concatenate([b for _, b in picks], axis=0)
        return jnp.dot(left, right, preferred_element_type=jnp.float32)

    far_base = blocks + home_blocks

    def near(i, _):
        picks = [(0, cur_v[cols[i, 0]])]
        picks += [(t, hist_av[jnp.maximum(cols[i, t] - blocks, 0)]) for t in range(1, home)]
        acc_a[i] = product(i, picks)
        acc_b[i] = product(i, [(t, hist_bv[jnp.maximum(cols[i, t] - blocks, 0)]) for t in range(1, home)])
        return 0

    lax.fori_loop(0, blocks, near, 0)

    def finish(i, acc_ref, pull_buf, w, number, factor_weight):
        far = product(i, [(t, pull_buf[jnp.maximum(cols[i, t] - far_base, 0)]) for t in range(home, tiles)])
        summed = acc_ref[i] + far
        mixed = (1.0 - restart) * summed + restart * zero_v[i].astype(jnp.float32)
        low = mixed.astype(jnp.bfloat16)
        prod = jnp.dot(low, w[...], preferred_element_type=jnp.float32)
        inner = (1.0 - factor_weight) * mixed + factor_weight * prod
        return jnp.maximum(inner, 0.0).astype(jnp.bfloat16), low

    whole(pull_a, D - 1, a_s, a_r).wait_recv()
    factor_two = math.log(strength / 2 + 1.0)
    factor_three = math.log(strength / 3 + 1.0)

    def second(i, _):
        fresh[i] = finish(i, acc_a, pull_a, w2_v, 2, factor_two)[0]
        return 0

    lax.fori_loop(0, blocks, second, 0)

    def fresh_copy(src, slot, target, k):
        return pltpu.make_async_remote_copy(
            src_ref=src, dst_ref=hist_out.at[slot], send_sem=f_s.at[k], recv_sem=f_r.at[k],
            device_id=(d, target), device_id_type=MESH,
        )

    keep = pltpu.make_async_copy(fresh, hist_out.at[r], out_sem.at[0])
    if R == 4:
        mate = r + 1 - 2 * lax.rem(r, 2)
        across = lax.rem(r + 2, R)
        sends = [fresh_copy(fresh, r, across, 0), fresh_copy(fresh, r, mate, 1)]
        forward = fresh_copy(hist_out.at[across], across, mate, 2)
    else:
        sends = [fresh_copy(fresh, r, lax.rem(r + 1 + k, R), k) for k in range(R - 1)]
        forward = None
    for c in sends:
        c.start()
    keep.start()

    def own_tile(i, _):
        acc_b[i] += product(i, [(0, fresh[cols[i, 0]])])
        return 0

    lax.fori_loop(0, blocks, own_tile, 0)
    whole(pull_b, D - 1, b_s, b_r).wait_recv()

    def third(i, _):
        out, low = finish(i, acc_b, pull_b, w3_v, 3, factor_three)
        out_v[i] = out
        low_v[i] = low
        return 0

    lax.fori_loop(0, blocks, third, 0)
    put = pltpu.make_async_copy(out_v, layer_out, out_sem.at[1])
    put.start()

    grad = factor_three * lax.dot_general(
        low_v[...].reshape(blocks * slots, feat), up_v[...].reshape(blocks * slots, feat),
        (((0,), (0,)), ((), ())), preferred_element_type=jnp.float32,
    )
    piece = g_send.shape[1]
    for c in range(N):
        g_send[c] = grad[c * piece:(c + 1) * piece, :]

    def scatter(k, _):
        t = lax.rem(me + 1 + k, N)
        pltpu.make_async_remote_copy(
            src_ref=g_send.at[t], dst_ref=g_recv.at[me], send_sem=g_s, recv_sem=g_r,
            device_id=(lax.div(t, R), lax.rem(t, R)), device_id_type=MESH,
        ).start()
        return 0

    lax.fori_loop(0, N - 1, scatter, 0)
    g_recv[me] = g_send[me]
    whole(g_recv, N - 1, g_s, g_r).wait_recv()

    g_part[...] = jnp.sum(g_recv[...], axis=0).astype(g_part.dtype)

    def spread(k, _):
        t = lax.rem(me + 1 + k, N)
        pltpu.make_async_remote_copy(
            src_ref=g_part, dst_ref=g_all.at[me], send_sem=p_s, recv_sem=p_r,
            device_id=(lax.div(t, R), lax.rem(t, R)), device_id_type=MESH,
        ).start()
        return 0

    lax.fori_loop(0, N - 1, spread, 0)
    g_all[me] = g_part[...]

    if forward is not None:
        sends[0].wait_recv()
        forward.start()
    whole(g_all, N - 1, p_s, p_r).wait_recv()
    grad_res[...] = g_all[...].astype(jnp.float32)

    if forward is not None:
        sends[1].wait_recv()
        forward.wait_recv()
        forward.wait_send()
    else:
        for c in sends:
            c.wait_recv()
    for c in sends:
        c.wait_send()
    keep.wait()
    put.wait()
    whole(ask, D - 1, idx_s, idx_r).wait_send()
    whole(send_a, D - 1, a_s, a_r).wait_send()
    whole(send_b, D - 1, b_s, b_r).wait_send()
    whole(g_send, N - 1, g_s, g_r).wait_send()
    whole(g_all, N - 1, p_s, p_r).wait_send()


def local(D, R, h_zero, h_prev, hist_a, hist_b, tile_vals, tile_cols, pull_rows, pull_counts,
          weight_two, weight_three, grad_out):
    blocks, tiles, tile = tile_vals.shape[:3]
    feat = hist_a.shape[1]
    N = D * R
    hist_blocks = hist_a.shape[0] // tile
    piece = feat // N
    bf, f32 = jnp.bfloat16, jnp.float32
    own = (blocks, tile, feat)
    hist = (hist_blocks, tile, feat)
    slots = pull_rows.shape[2]
    pulled = (D, slots, feat)
    group = 4 if D % 4 == 0 else 1
    vm = pltpu.VMEM
    dma = pltpu.SemaphoreType.DMA
    any_spec = pl.BlockSpec(memory_space=pl.ANY)
    smem = pl.BlockSpec(memory_space=pltpu.SMEM)
    vspec = pl.BlockSpec(memory_space=pltpu.VMEM)
    out3, fresh, grad = pl.pallas_call(
        functools.partial(kernel, D, R),
        out_shape=(
            jax.ShapeDtypeStruct(own, bf),
            jax.ShapeDtypeStruct((R,) + own, bf),
            jax.ShapeDtypeStruct((N, piece, feat), f32),
        ),
        in_specs=[smem, smem, vspec] + [any_spec] * 8,
        out_specs=(any_spec, any_spec, vspec),
        scratch_shapes=[
            vm(own, bf), vm(own, bf), vm(hist, bf), vm(hist, bf), vm(tile_vals.shape, bf),
            vm((feat, feat), bf), vm((feat, feat), bf), vm(own, bf),
            vm((D, 1, slots), jnp.int32), vm((D, 1, slots), jnp.int32),
            vm((D, slots, slots), jnp.int32),
            vm(pulled, bf), vm(pulled, bf), vm(pulled, bf), vm(pulled, bf),
            vm((group * slots, feat), f32), vm(own, f32), vm(own, f32),
            vm(own, bf), vm(own, bf), vm(own, bf),
            vm((N, piece, feat), f32), vm((N, piece, feat), f32),
            vm((piece, feat), bf), vm((N, piece, feat), bf),
            dma((8,)), dma, dma, dma, dma, dma, dma,
            dma((max(R - 1, 3),)), dma((max(R - 1, 3),)), dma((2,)), dma, dma, dma, dma,
        ],
        compiler_params=pltpu.CompilerParams(
            collective_id=0, has_side_effects=True, vmem_limit_bytes=60 * 1024 * 1024
        ),
    )(
        tile_cols, pull_counts, pull_rows,
        h_zero.reshape(own), h_prev.reshape(own), hist_a.reshape(hist), hist_b.reshape(hist),
        tile_vals, weight_two, weight_three, grad_out.reshape(own),
    )
    return (
        out3.reshape(h_zero.shape),
        fresh.reshape(R * h_zero.shape[0], feat),
        grad.reshape(feat, feat),
    )


def solution(mesh):
    both = ("dev", "rep")
    return jax.shard_map(
        functools.partial(local, mesh.shape["dev"], mesh.shape["rep"]),
        mesh=mesh,
        in_specs=(
            P(both, None), P(both, None), P("dev", None), P("dev", None),
            P(both, None, None, None), P(both, None), P(both, None, None), P(both, None),
            P(), P(), P(both, None),
        ),
        out_specs=(P(both, None), P("dev", None), P()),
        check_vma=False,
    )
```

```python
import functools
import math

import jax
import jax.numpy as jnp
from jax import lax
from jax.experimental import pallas as pl
from jax.experimental.pallas import tpu as pltpu
from jax.sharding import PartitionSpec as P

restart = 0.1
strength = 0.5
MESH = pl.DeviceIdType.MESH


def kernel(
    D, R,
    cols, counts, rows_in,
    h_zero, h_prev, hist_a, hist_b, tile_vals, w_two, w_three, grad_out,
    layer_out, hist_out, grad_res,
    zero_v, cur_v, hist_av, hist_bv, vals_v, w2_v, w3_v, up_v,
    ask, asked, col, send_a, send_b, pull_a, pull_b, acc, acc_a, acc_b,
    fresh_v, low_v, g_send, g_mate, g_recv, g_part, g_all,
    local_sem, idx_s, idx_r, a_s, a_r, b_s, b_r, f_s, f_r, m_s, m_r, g_s, g_r, p_s, p_r,
):
    N = D * R
    d = lax.axis_index("dev")
    r = lax.axis_index("rep")
    me = d * R + r
    slots = rows_in.shape[2]
    feat = hist_av.shape[2]
    blocks = vals_v.shape[0]
    tiles = vals_v.shape[1]
    home = 4
    home_blocks = hist_av.shape[0]

    loads = [
        (hist_a, hist_av), (tile_vals, vals_v), (h_prev, cur_v), (hist_b, hist_bv),
        (h_zero, zero_v), (w_two, w2_v), (w_three, w3_v), (grad_out, up_v),
    ]
    copies = [pltpu.make_async_copy(s, t, local_sem.at[i]) for i, (s, t) in enumerate(loads)]
    for c in copies:
        c.start()

    barrier = pltpu.get_barrier_semaphore()

    def greet(k, _):
        t = lax.rem(me + 1 + k, N)
        pl.semaphore_signal(
            barrier, inc=1, device_id=(lax.div(t, R), lax.rem(t, R)), device_id_type=MESH
        )
        return 0

    lax.fori_loop(0, N - 1, greet, 0)

    lane = lax.broadcasted_iota(jnp.int32, (1, slots), 1)

    def mask_rows(p, _):
        ask[p] = jnp.where(lane < counts[0, p], rows_in[0, pl.ds(p, 1), :], -1)
        return 0

    lax.fori_loop(0, D, mask_rows, 0)
    pl.semaphore_wait(barrier, N - 1)

    def offset(j):
        return D // 2 + lax.div(j + 1, 2) * (1 - 2 * lax.rem(j, 2))

    def send_rows(j, _):
        p = lax.rem(d + offset(j), D)
        pltpu.make_async_remote_copy(
            src_ref=ask.at[p], dst_ref=asked.at[d], send_sem=idx_s, recv_sem=idx_r,
            device_id=(p, r), device_id_type=MESH,
        ).start()
        return 0

    lax.fori_loop(0, D - 1, send_rows, 0)
    asked[d] = ask[d]

    def whole(ref, n, s, q):
        part = ref.at[pl.ds(0, n)]
        return pltpu.make_async_remote_copy(
            src_ref=part, dst_ref=part, send_sem=s, recv_sem=q,
            device_id=(lax.rem(d + 1, D), r), device_id_type=MESH,
        )

    whole(asked, D - 1, idx_s, idx_r).wait_recv()

    def column(j, _):
        q = lax.rem(d + D - offset(j), D)
        col[j] = jnp.broadcast_to(asked[q], (slots, slots)).T
        return 0

    lax.fori_loop(0, D, column, 0)

    group = 2 if D % 2 == 0 else 1
    chunk_blocks = 8
    depth = chunk_blocks * slots
    lanes = lax.broadcasted_iota(jnp.int32, (group * slots, depth), 1)

    def gather(table, send_buf, pull_buf, s, q_sem):
        def one_group(g, _):
            keys = col[pl.ds(g * group, group)].reshape(group * slots, slots)
            wide = jnp.concatenate([keys] * chunk_blocks, axis=1)

            def one_chunk(k, _):
                hot = jnp.where(wide - k * depth == lanes, 1.0, 0.0).astype(jnp.bfloat16)
                part = table[pl.ds(k * chunk_blocks, chunk_blocks)].reshape(depth, feat)
                found = jnp.dot(hot, part, preferred_element_type=jnp.float32)

                @pl.when(k == 0)
                def _():
                    acc[...] = found

                @pl.when(k > 0)
                def _():
                    acc[...] += found

                return 0

            lax.fori_loop(0, home_blocks // chunk_blocks, one_chunk, 0)
            send_buf[pl.ds(g * group, group)] = (
                acc[...].astype(jnp.bfloat16).reshape(group, slots, feat)
            )

            def send_one(i, _):
                j = g * group + i

                @pl.when(j < D - 1)
                def _():
                    q = lax.rem(d + D - offset(j), D)
                    pltpu.make_async_remote_copy(
                        src_ref=send_buf.at[j], dst_ref=pull_buf.at[d], send_sem=s, recv_sem=q_sem,
                        device_id=(q, r), device_id_type=MESH,
                    ).start()

                return 0

            lax.fori_loop(0, group, send_one, 0)
            return 0

        lax.fori_loop(0, D // group, one_group, 0)
        pull_buf[d] = send_buf[D - 1]

    copies[0].wait()
    gather(hist_av, send_a, pull_a, a_s, a_r)
    copies[3].wait()
    gather(hist_bv, send_b, pull_b, b_s, b_r)
    for i in (1, 2, 4, 5, 6, 7):
        copies[i].wait()

    def product(i, picks):
        left = jnp.concatenate([vals_v[i, t] for t, _ in picks], axis=1)
        right = jnp.concatenate([b for _, b in picks], axis=0)
        return jnp.dot(left, right, preferred_element_type=jnp.float32)

    far_base = blocks + home_blocks

    def near(i, _):
        picks = [(0, cur_v[cols[i, 0]])]
        picks += [(t, hist_av[jnp.maximum(cols[i, t] - blocks, 0)]) for t in range(1, home)]
        acc_a[i] = product(i, picks)
        acc_b[i] = product(i, [(t, hist_bv[jnp.maximum(cols[i, t] - blocks, 0)]) for t in range(1, home)])
        return 0

    lax.fori_loop(0, blocks, near, 0)

    def finish(i, acc_ref, pull_buf, w, number, factor_weight):
        far = product(i, [(t, pull_buf[jnp.maximum(cols[i, t] - far_base, 0)]) for t in range(home, tiles)])
        summed = acc_ref[i] + far
        mixed = (1.0 - restart) * summed + restart * zero_v[i].astype(jnp.float32)
        low = mixed.astype(jnp.bfloat16)
        prod = jnp.dot(low, w[...], preferred_element_type=jnp.float32)
        inner = (1.0 - factor_weight) * mixed + factor_weight * prod
        return jnp.maximum(inner, 0.0).astype(jnp.bfloat16), low

    whole(pull_a, D - 1, a_s, a_r).wait_recv()
    factor_two = math.log(strength / 2 + 1.0)
    factor_three = math.log(strength / 3 + 1.0)

    def second(i, _):
        rows = finish(i, acc_a, pull_a, w2_v, 2, factor_two)[0]
        fresh_v[i] = rows
        hist_out[r, i] = rows
        return 0

    lax.fori_loop(0, blocks, second, 0)

    def fresh_copy(src, slot, target, k):
        return pltpu.make_async_remote_copy(
            src_ref=src, dst_ref=hist_out.at[slot], send_sem=f_s.at[k], recv_sem=f_r.at[k],
            device_id=(d, target), device_id_type=MESH,
        )

    fresh = hist_out.at[r]
    side = lax.rem(r, 2)
    mate = r + 1 - 2 * side
    if R == 4:
        across = lax.rem(r + 2, R)
        sends = [fresh_copy(fresh, r, across, 0), fresh_copy(fresh, r, mate, 1)]
        forward = fresh_copy(hist_out.at[across], across, mate, 2)
    else:
        sends = [fresh_copy(fresh, r, lax.rem(r + 1 + k, R), k) for k in range(R - 1)]
        forward = None
    for c in sends:
        c.start()

    def own_tile(i, _):
        acc_b[i] += product(i, [(0, fresh_v[cols[i, 0]])])
        return 0

    lax.fori_loop(0, blocks, own_tile, 0)
    whole(pull_b, D - 1, b_s, b_r).wait_recv()

    def third(i, _):
        out, low = finish(i, acc_b, pull_b, w3_v, 3, factor_three)
        layer_out[i] = out
        low_v[i] = low
        return 0

    lax.fori_loop(0, blocks, third, 0)

    grad = factor_three * lax.dot_general(
        low_v[...].reshape(blocks * slots, feat), up_v[...].reshape(blocks * slots, feat),
        (((0,), (0,)), ((), ())), preferred_element_type=jnp.float32,
    )
    half = N // 2
    piece = g_send.shape[2]
    for c in range(N):
        g_send[c // half, c % half] = grad[c * piece:(c + 1) * piece, :]
    place = d * (R // 2) + lax.div(r, 2)
    to_mate = pltpu.make_async_remote_copy(
        src_ref=g_send.at[1 - side], dst_ref=g_mate, send_sem=m_s, recv_sem=m_r,
        device_id=(d, mate), device_id_type=MESH,
    )
    to_mate.start()
    to_mate.wait_recv()
    g_mate[...] += g_send[side]

    def scatter(k, _):
        t = lax.rem(place + 1 + k, half)
        pltpu.make_async_remote_copy(
            src_ref=g_mate.at[t], dst_ref=g_recv.at[place], send_sem=g_s, recv_sem=g_r,
            device_id=(lax.div(t, R // 2), 2 * lax.rem(t, R // 2) + side), device_id_type=MESH,
        ).start()
        return 0

    lax.fori_loop(0, half - 1, scatter, 0)
    g_recv[place] = g_mate[place]
    if forward is not None:
        sends[0].wait_recv()
        forward.start()
    whole(g_recv, half - 1, g_s, g_r).wait_recv()

    g_part[...] = jnp.sum(g_recv[...], axis=0).astype(g_part.dtype)
    mine = side * half + place

    def spread(k, _):
        t = lax.rem(me + 1 + k, N)
        pltpu.make_async_remote_copy(
            src_ref=g_part, dst_ref=g_all.at[mine], send_sem=p_s, recv_sem=p_r,
            device_id=(lax.div(t, R), lax.rem(t, R)), device_id_type=MESH,
        ).start()
        return 0

    lax.fori_loop(0, N - 1, spread, 0)
    g_all[mine] = g_part[...]
    whole(g_all, N - 1, p_s, p_r).wait_recv()
    grad_res[...] = g_all[...].astype(jnp.float32)

    if forward is not None:
        sends[1].wait_recv()
        forward.wait_recv()
        forward.wait_send()
    else:
        for c in sends:
            c.wait_recv()
    for c in sends:
        c.wait_send()
    whole(ask, D - 1, idx_s, idx_r).wait_send()
    whole(send_a, D - 1, a_s, a_r).wait_send()
    whole(send_b, D - 1, b_s, b_r).wait_send()
    to_mate.wait_send()
    whole(g_recv, half - 1, g_s, g_r).wait_send()
    whole(g_all, N - 1, p_s, p_r).wait_send()


def hand_over(parts, *refs):
    sources, targets, sem = refs[:3], refs[3:6], refs[6]
    outs = []
    for n, src, dst in zip(parts, sources, targets):
        rows = src.shape[0] // n
        for i in range(n):
            at = pl.ds(i * rows, rows)
            outs.append(pltpu.make_async_copy(src.at[at], dst.at[at], sem.at[len(outs)]))
    for c in outs:
        c.start()
    for c in outs:
        c.wait()


def local(D, R, h_zero, h_prev, hist_a, hist_b, tile_vals, tile_cols, pull_rows, pull_counts,
          weight_two, weight_three, grad_out):
    blocks, tiles, tile = tile_vals.shape[:3]
    feat = hist_a.shape[1]
    N = D * R
    hist_blocks = hist_a.shape[0] // tile
    piece = feat // N
    bf, f32 = jnp.bfloat16, jnp.float32
    own = (blocks, tile, feat)
    hist = (hist_blocks, tile, feat)
    slots = pull_rows.shape[2]
    pulled = (D, slots, feat)
    group = 2 if D % 2 == 0 else 1
    vm = pltpu.VMEM
    dma = pltpu.SemaphoreType.DMA
    any_spec = pl.BlockSpec(memory_space=pl.ANY)
    smem = pl.BlockSpec(memory_space=pltpu.SMEM)
    vspec = pl.BlockSpec(memory_space=pltpu.VMEM)
    grant = 20 * 2**20 + D * slots * (8 * feat + 4 * slots)
    out3, fresh, grad = pl.pallas_call(
        functools.partial(kernel, D, R),
        out_shape=(
            jax.ShapeDtypeStruct(own, bf),
            jax.ShapeDtypeStruct((R,) + own, bf),
            jax.ShapeDtypeStruct((N, piece, feat), f32),
        ),
        in_specs=[smem, smem, vspec] + [any_spec] * 8,
        out_specs=(vspec, vspec, vspec),
        scratch_shapes=[
            vm(own, bf), vm(own, bf), vm(hist, bf), vm(hist, bf), vm(tile_vals.shape, bf),
            vm((feat, feat), bf), vm((feat, feat), bf), vm(own, bf),
            vm((D, 1, slots), jnp.int32), vm((D, 1, slots), jnp.int32),
            vm((D, slots, slots), jnp.int32),
            vm(pulled, bf), vm(pulled, bf), vm(pulled, bf), vm(pulled, bf),
            vm((group * slots, feat), f32), vm(own, f32), vm(own, f32),
            vm(own, bf), vm(own, bf),
            vm((2, N // 2, piece, feat), f32), vm((N // 2, piece, feat), f32),
            vm((N // 2, piece, feat), f32),
            vm((piece, feat), bf), vm((N, piece, feat), bf),
            dma((8,)), dma, dma, dma, dma, dma, dma,
            dma((max(R - 1, 3),)), dma((max(R - 1, 3),)), dma, dma, dma, dma, dma, dma,
        ],
        compiler_params=pltpu.CompilerParams(
            collective_id=0, has_side_effects=True, vmem_limit_bytes=grant
        ),
    )(
        *[
            pltpu.with_memory_space_constraint(x, pltpu.HBM)
            for x in (
                tile_cols, pull_counts, pull_rows, h_zero.reshape(own), h_prev.reshape(own),
                hist_a.reshape(hist), hist_b.reshape(hist), tile_vals, weight_two, weight_three,
                grad_out.reshape(own),
            )
        ]
    )
    flat = (
        out3.reshape(h_zero.shape),
        fresh.reshape(R * h_zero.shape[0], feat),
        grad.reshape(feat, feat),
    )
    parts = (4, 8, 1)
    return pl.pallas_call(
        functools.partial(hand_over, parts),
        out_shape=tuple(jax.ShapeDtypeStruct(x.shape, x.dtype) for x in flat),
        in_specs=[vspec] * 3,
        out_specs=(any_spec,) * 3,
        scratch_shapes=[dma((sum(parts),))],
        compiler_params=pltpu.CompilerParams(vmem_limit_bytes=8 * 1024 * 1024),
    )(*flat)


def solution(mesh):
    both = ("dev", "rep")
    return jax.shard_map(
        functools.partial(local, mesh.shape["dev"], mesh.shape["rep"]),
        mesh=mesh,
        in_specs=(
            P(both, None), P(both, None), P("dev", None), P("dev", None),
            P(both, None, None, None), P(both, None), P(both, None, None), P(both, None),
            P(), P(), P(both, None),
        ),
        out_specs=(P(both, None), P("dev", None), P()),
        check_vma=False,
    )
```
